16 devices in a mesh: dp: 4 (over y, z, core), tp: 4 (over x).
Axes of the slice: x: 4, y: 2, z: 1, core: 2. Of those that a mesh axis runs over, the one named last changes fastest.
The devices are a block of a 4x4x8 slice.
Arguments:
- x: bfloat16 [512, 4096], P('dp'), parts along dimension 0
- w_gate: bfloat16 [4096, 10240], P(None, 'tp')
- w_up: bfloat16 [4096, 10240], P(None, 'tp')
- w_down: bfloat16 [10240, 4096], P('tp')
Outputs:
- output: bfloat16 [512, 4096], P('dp'), parts along dimension 0
There are 4 independent parts. The reference program is written for one: setup_inputs(seed, part) draws one part's arguments, and reference() takes and returns one part's arrays. A program takes and returns all parts, laid end to end along the dimension named above; an argument that names none is the same for every part.
All inputs are finite; a program needn't handle non-finite values.
Results may differ from the reference program's by a relative error of at most 0.016.
Values are sent between devices in bfloat16 or wider.
A program may use at most 768 MiB of HBM per device.

```python
import jax
import jax.numpy as jnp

ROWS = 128
D = 4096
FF = 10240


def setup_inputs(seed: int = 0, part: int = 0) -> dict:
    kx, kg, ku, kd = jax.random.split(jax.random.key(seed), 4)
    drawn = {
        "x": jax.random.normal(jax.random.fold_in(kx, part), (ROWS, D), jnp.float32),
        "w_gate": jax.random.normal(kg, (D, FF), jnp.float32) * D**-0.5,
        "w_up": jax.random.normal(ku, (D, FF), jnp.float32) * D**-0.5,
        "w_down": jax.random.normal(kd, (FF, D), jnp.float32) * FF**-0.5,
    }
    return {k: v.astype(jnp.bfloat16) for k, v in drawn.items()}


def reference(x, w_gate, w_up, w_down):
    gate = jnp.dot(x, w_gate, preferred_element_type=jnp.float32)
    up = jnp.dot(x, w_up, preferred_element_type=jnp.float32)
    hidden = (jax.nn.gelu(gate) * up).astype(jnp.bfloat16)
    return jnp.dot(hidden, w_down, preferred_element_type=jnp.float32).astype(jnp.bfloat16)
```

```python
import functools

import jax
import jax.numpy as jnp
from jax import lax
from jax.experimental import pallas as pl
from jax.experimental.pallas import tpu as pltpu
from jax.sharding import PartitionSpec as P

MESH = pl.DeviceIdType.MESH
BF16 = jnp.bfloat16
F32 = jnp.float32
TK = 256
TN = 256
XP = 4
FAR, NEAR, CARRY = 0, 1, 2
RIGHT, LEFT = 0, 1


def kernel(
    n, x_hbm, wg_hbm, wu_hbm, wd_hbm, y_ref,
    xv, wgu, wd, gacc, hid, yacc, stage, recv, yb,
    x_sem, xs_send, xs_recv, w_sem, d_sem, h_send, h_recv,
    rs_send, rs_recv, ag_send, ag_recv, fw_send, fw_recv, own_send, own_recv,
):
    t = lax.axis_index("tp")
    g = lax.axis_index("dp")
    core = lax.rem(g, 2)
    base = g - core
    other = base + 1 - core
    right, left = lax.rem(t + 1, n), lax.rem(t + n - 1, n)
    far = lax.rem(t + 2, n)
    rows, depth = x_hbm.shape
    half = wg_hbm.shape[1] // 2
    steps = half // TK
    cols = wd_hbm.shape[1] // 2
    block = cols // n
    to = (right, left)

    def dev(tp, dp):
        return {"tp": tp, "dp": dp}

    def remote(src, dst, send, rcv, device):
        return pltpu.make_async_remote_copy(
            src_ref=src, dst_ref=dst, send_sem=send, recv_sem=rcv,
            device_id=device, device_id_type=MESH,
        )

    mine = pl.ds(pl.multiple_of(core * rows, rows), rows)
    his = pl.ds(pl.multiple_of((1 - core) * rows, rows), rows)
    x_load = pltpu.make_async_copy(x_hbm, xv.at[mine, :], x_sem)
    x_load.start()
    first = core * half
    w_loads = []
    for j in range(steps):
        at = pl.ds(pl.multiple_of(first + j * TK, TK), TK)
        w_loads.append((
            pltpu.make_async_copy(wg_hbm.at[:, at], wgu.at[j, :, :TK], w_sem.at[j, 0]),
            pltpu.make_async_copy(wu_hbm.at[:, at], wgu.at[j, :, TK:], w_sem.at[j, 1]),
        ))
    order = ((far, 0), (far, 1), (right, 1), (left, 0), (right, 0), (left, 1), (t, 0), (t, 1))
    d_loads = []
    for s, (owner, h) in enumerate(order):
        at = pl.ds(pl.multiple_of(core * cols + owner * block + h * TN, TN), TN)
        d_loads.append((
            pltpu.make_async_copy(
                wd_hbm.at[pl.ds(pl.multiple_of(core * half, half), half), at],
                wd.at[s, :half, :], d_sem.at[s, 0]),
            pltpu.make_async_copy(
                wd_hbm.at[pl.ds(pl.multiple_of((1 - core) * half, half), half), at],
                wd.at[s, half:, :], d_sem.at[s, 1]),
        ))
    for pair in w_loads + d_loads:
        for copy in pair:
            copy.start()

    barrier = pltpu.get_barrier_semaphore()
    partners = [dev(t, other)] + [dev(a, b) for a in to for b in (g, other)]
    for p in partners:
        pl.semaphore_signal(barrier, inc=1, device_id=p, device_id_type=MESH)
    pl.semaphore_wait(barrier, len(partners))

    x_load.wait()
    x_moves = []
    for k in range(XP):
        at = pl.ds(k * (depth // XP), depth // XP)
        x_moves.append(remote(xv.at[mine, at], xv.at[mine, at], xs_send.at[k], xs_recv.at[k], dev(t, other)))
        x_moves[-1].start()

    def gate_up(j, r):
        gacc[j % 2, r, :] = jnp.dot(xv[r, :], wgu[j], preferred_element_type=F32)

    h_moves = []

    def activate(j):
        a = gacc[j % 2]
        at = pl.ds(j * TK, TK)
        hid[:, at] = (jax.nn.gelu(a[:, :TK]) * a[:, TK:]).astype(BF16)
        h_moves.append(remote(
            hid.at[:, at], hid.at[:, pl.ds(half + j * TK, TK)], h_send.at[j], h_recv.at[j], dev(t, other)))
        h_moves[-1].start()

    for j in range(steps):
        for copy in w_loads[j]:
            copy.wait()
        if j == 0:
            gate_up(0, mine)
            for k in range(XP):
                at = pl.ds(k * (depth // XP), depth // XP)
                remote(xv.at[his, at], xv.at[his, at], xs_send.at[k], xs_recv.at[k], dev(t, other)).wait_recv()
            gate_up(0, his)
        else:
            gate_up(j, slice(None))
            activate(j - 1)
    activate(steps - 1)
    for move in h_moves:
        move.wait_recv()

    sends = []

    def hop(kind, d, p):
        i = (kind * 2 + d) * 2 + p
        return remote(stage.at[i], recv.at[i], rs_send.at[i], rs_recv.at[i], dev(to[d], g))

    def put(kind, d, p, v):
        i = (kind * 2 + d) * 2 + p
        stage[i] = v.astype(BF16)
        move = hop(kind, d, p)
        move.start()
        sends.append(move)

    def part(p):
        return slice(p * rows, (p + 1) * rows)

    for s, (kind, d) in enumerate(((FAR, RIGHT), (FAR, LEFT), (NEAR, RIGHT), (NEAR, LEFT))):
        for copy in d_loads[s]:
            copy.wait()
        v = jnp.dot(hid[...], wd[s], preferred_element_type=F32)
        if kind == FAR:
            for p in (0, 1):
                put(kind, d, p, v[part(p)])
        else:
            put(kind, d, 0, v[part(0)])
            i = (kind * 2 + d) * 2 + 1
            stage[i] = v[part(1)].astype(BF16)
    for s in range(4, 8):
        for copy in d_loads[s]:
            copy.wait()
        yacc[s - 4] = jnp.dot(hid[...], wd[s], preferred_element_type=F32)

    def got(kind, d, p):
        hop(kind, d, p).wait_recv()
        return recv[(kind * 2 + d) * 2 + p].astype(F32)

    for p in (0, 1):
        for d in (RIGHT, LEFT):
            put(CARRY, d, p, yacc[d, part(p), :] + got(FAR, d, p))
        if p == 0:
            for d in (RIGHT, LEFT):
                move = hop(NEAR, d, 1)
                move.start()
                sends.append(move)

    def place(k, owner, h, width):
        return pl.ds(pl.multiple_of(k * cols + owner * block + h * TN, TN), width)

    for p in (0, 1):
        yb[p, :, :TN] = (yacc[2, part(p), :] + got(CARRY, RIGHT, p) + got(NEAR, LEFT, p)).astype(BF16)
        for d, h in ((RIGHT, 0),):
            move = remote(yb.at[p, :, pl.ds(h * TN, TN)], y_ref.at[:, place(core, t, h, TN)],
                          ag_send.at[p, d, h], ag_recv.at[d, h, core], dev(to[d], base + p))
            move.start()
            sends.append(move)
        yb[p, :, TN:] = (yacc[3, part(p), :] + got(CARRY, LEFT, p) + got(NEAR, RIGHT, p)).astype(BF16)
        for d, h in ((LEFT, 1), (RIGHT, 1), (LEFT, 0)):
            move = remote(yb.at[p, :, pl.ds(h * TN, TN)], y_ref.at[:, place(core, t, h, TN)],
                          ag_send.at[p, d, h], ag_recv.at[d, h, core], dev(to[d], base + p))
            move.start()
            sends.append(move)

        @pl.when(core == p)
        def _():
            y_ref[:, place(core, t, 0, block)] = yb[p]

        @pl.when(core != p)
        def _():
            remote(yb.at[p], y_ref.at[:, place(core, t, 0, block)], own_send, own_recv, dev(t, other)).start()

    def landed(d, h, k):
        owner = (left, right)[d]
        at = place(k, owner, h, TN)
        return remote(y_ref.at[:, at], y_ref.at[:, at], ag_send.at[0, d, h], ag_recv.at[d, h, k], dev(to[d], g))

    for k in (0, 1):
        for d, h in ((RIGHT, 0), (LEFT, 1)):
            landed(d, h, k).wait_recv()
            at = place(k, (left, right)[d], h, TN)
            move = remote(y_ref.at[:, at], y_ref.at[:, at], fw_send.at[d, k], fw_recv.at[d, k], dev(to[d], g))
            move.start()
            sends.append(move)
    for k in (0, 1):
        for d, h in ((RIGHT, 1), (LEFT, 0)):
            landed(d, h, k).wait_recv()
    at = place(1 - core, t, 0, block)
    sib = remote(yb.at[0], y_ref.at[:, at], own_send, own_recv, dev(t, other))
    sib.wait_recv()
    for k in (0, 1):
        for d, h in ((RIGHT, 0), (LEFT, 1)):
            at = place(k, far, h, TN)
            remote(y_ref.at[:, at], y_ref.at[:, at], fw_send.at[d, k], fw_recv.at[d, k], dev(to[d], g)).wait_recv()
    sib.wait_send()
    for move in x_moves + h_moves + sends:
        move.wait_send()


def solution(mesh):
    n = mesh.shape["tp"]

    def step(x, w_gate, w_up, w_down):
        rows, depth = x.shape
        hidden, out = w_down.shape
        half, cols = hidden // 2, out // 2
        steps, pieces = half // TK, cols // TN
        DMA = pltpu.SemaphoreType.DMA
        any_spec = pl.BlockSpec(memory_space=pl.ANY)
        return pl.pallas_call(
            functools.partial(kernel, n),
            out_shape=jax.ShapeDtypeStruct((rows, out), BF16),
            in_specs=[any_spec] * 4,
            out_specs=pl.BlockSpec(memory_space=pltpu.VMEM),
            scratch_shapes=[
                pltpu.VMEM((2 * rows, depth), BF16),
                pltpu.VMEM((steps, depth, 2 * TK), BF16),
                pltpu.VMEM((pieces, hidden, TN), BF16),
                pltpu.VMEM((2, 2 * rows, 2 * TK), F32),
                pltpu.VMEM((2 * rows, hidden), BF16),
                pltpu.VMEM((4, 2 * rows, TN), F32),
                pltpu.VMEM((12, rows, TN), BF16),
                pltpu.VMEM((12, rows, TN), BF16),
                pltpu.VMEM((2, rows, 2 * TN), BF16),
                DMA, DMA((XP,)), DMA((XP,)), DMA((steps, 2)), DMA((pieces, 2)), DMA((steps,)), DMA((steps,)),
                DMA((12,)), DMA((12,)), DMA((2, 2, 2)), DMA((2, 2, 2)), DMA((2, 2)), DMA((2, 2)), DMA, DMA,
            ],
            compiler_params=pltpu.CompilerParams(
                collective_id=0, has_side_effects=True, vmem_limit_bytes=56 * 1024 * 1024
            ),
        )(x, w_gate, w_up, w_down)

    return jax.shard_map(
        step,
        mesh=mesh,
        in_specs=(P("dp", None), P(None, "tp"), P(None, "tp"), P("tp", None)),
        out_specs=P("dp", None),
        check_vma=False,
    )
```

```python
import functools

import jax
import jax.numpy as jnp
from jax import lax
from jax.experimental import pallas as pl
from jax.experimental.pallas import tpu as pltpu
from jax.sharding import PartitionSpec as P

MESH = pl.DeviceIdType.MESH
BF16 = jnp.bfloat16
F32 = jnp.float32
TK = 256
TN = 256
XP = 4
FAR, NEAR, CARRY = 0, 1, 2
RIGHT, LEFT = 0, 1


def kernel(
    n, x_hbm, wg_hbm, wu_hbm, wd_hbm, y_ref,
    xv, wgu, wd, gacc, hid, yacc, carry, stage, recv, yb,
    x_sem, xs_send, xs_recv, w_sem, d_sem, h_send, h_recv,
    rs_send, rs_recv, ag_send, ag_recv, fw_send, fw_recv, own_send, own_recv,
):
    t = lax.axis_index("tp")
    g = lax.axis_index("dp")
    core = lax.rem(g, 2)
    base = g - core
    other = base + 1 - core
    right, left = lax.rem(t + 1, n), lax.rem(t + n - 1, n)
    far = lax.rem(t + 2, n)
    rows, depth = x_hbm.shape
    half = wg_hbm.shape[1] // 2
    steps = half // TK
    cols = wd_hbm.shape[1] // 2
    block = cols // n
    to = (right, left)

    def dev(tp, dp):
        return {"tp": tp, "dp": dp}

    def remote(src, dst, send, rcv, device):
        return pltpu.make_async_remote_copy(
            src_ref=src, dst_ref=dst, send_sem=send, recv_sem=rcv,
            device_id=device, device_id_type=MESH,
        )

    mine = pl.ds(pl.multiple_of(core * rows, rows), rows)
    his = pl.ds(pl.multiple_of((1 - core) * rows, rows), rows)
    pieces = [pl.ds(k * (depth // XP), depth // XP) for k in range(XP)]
    x_loads = [pltpu.make_async_copy(x_hbm.at[:, at], xv.at[mine, at], x_sem.at[k]) for k, at in enumerate(pieces)]
    for copy in x_loads:
        copy.start()
    first = core * half
    w_loads = []
    for j in range(steps):
        at = pl.ds(pl.multiple_of(first + j * TK, TK), TK)
        w_loads.append((
            pltpu.make_async_copy(wg_hbm.at[:, at], wgu.at[j, :, :TK], w_sem.at[j, 0]),
            pltpu.make_async_copy(wu_hbm.at[:, at], wgu.at[j, :, TK:], w_sem.at[j, 1]),
        ))
    order = (far, right, left, t)
    d_loads = []
    for s, owner in enumerate(order):
        at = pl.ds(pl.multiple_of(core * cols + owner * block, block), block)
        d_loads.append((
            pltpu.make_async_copy(
                wd_hbm.at[pl.ds(pl.multiple_of(core * half, half), half), at],
                wd.at[s, :half, :], d_sem.at[s, 0]),
            pltpu.make_async_copy(
                wd_hbm.at[pl.ds(pl.multiple_of((1 - core) * half, half), half), at],
                wd.at[s, half:, :], d_sem.at[s, 1]),
        ))

    def start(copies):
        for copy in copies:
            copy.start(priority=1)

    for pair in w_loads:
        start(pair)

    barrier = pltpu.get_barrier_semaphore()
    partners = [dev(t, other)] + [dev(a, b) for a in to for b in (g, other)]
    for p in partners:
        pl.semaphore_signal(barrier, inc=1, device_id=p, device_id_type=MESH)
    pl.semaphore_wait(barrier, len(partners))
    x_moves = []
    for k, at in enumerate(pieces):
        x_loads[k].wait()
        x_moves.append(remote(xv.at[mine, at], xv.at[mine, at], xs_send.at[k], xs_recv.at[k], dev(t, other)))
        x_moves[-1].start()

    def gate_up(j, r):
        gacc[j % 2, r, :] = jnp.dot(xv[r, :], wgu[j], preferred_element_type=F32)

    h_moves = []

    def activate(j):
        a = gacc[j % 2]
        at = pl.ds(j * TK, TK)
        hid[:, at] = (jax.nn.gelu(a[:, :TK]) * a[:, TK:]).astype(BF16)
        h_moves.append(remote(
            hid.at[:, at], hid.at[:, pl.ds(half + j * TK, TK)], h_send.at[j], h_recv.at[j], dev(t, other)))
        h_moves[-1].start()

    def wait(copies, name):
        with jax.named_scope(name):
            for copy in copies:
                copy.wait()

    wait(w_loads[0], "w0")
    gate_up(0, mine)
    wait(w_loads[1], "w1")
    for k, at in enumerate(pieces):
        with jax.named_scope("waitx"):
            remote(xv.at[his, at], xv.at[his, at], xs_send.at[k], xs_recv.at[k], dev(t, other)).wait_recv()
    gate_up(0, his)
    for j in range(1, steps):
        if j > 1:
            wait(w_loads[j], f"w{j}")
            start(d_loads[j - 2])
            if j == steps - 1:
                start(d_loads[3])
        gate_up(j, slice(None))
        activate(j - 1)
    activate(steps - 1)

    sends = []

    def hop(kind, d, p):
        i = (kind * 2 + d) * 2 + p
        return remote(stage.at[i], recv.at[i], rs_send.at[i], rs_recv.at[i], dev(to[d], g))

    def put(kind, d, p, v):
        i = (kind * 2 + d) * 2 + p
        stage[i] = v.astype(BF16)

    def send(kind, d, p):
        move = hop(kind, d, p)
        move.start()
        sends.append(move)

    def part(p):
        return slice(p * rows, (p + 1) * rows)

    most = 2 * half - TK
    wait(d_loads[0], "d0")
    for j in range(steps - 1):
        with jax.named_scope("h"):
            h_moves[j].wait_recv()
    yacc[...] = jnp.dot(hid[:, :most], wd[0, :most, :], preferred_element_type=F32)
    with jax.named_scope("hlast"):
        h_moves[steps - 1].wait_recv()
    v = yacc[...] + jnp.dot(hid[:, most:], wd[0, most:, :], preferred_element_type=F32)
    for p in (0, 1):
        for d in (RIGHT, LEFT):
            put(FAR, d, p, v[part(p), d * TN : (d + 1) * TN])
            send(FAR, d, p)
    for d in (RIGHT, LEFT):
        wait(d_loads[1 + d], f"d{1 + d}")
        v = jnp.dot(hid[...], wd[1 + d], preferred_element_type=F32)
        for p in (0, 1):
            put(NEAR, d, p, v[part(p), (1 - d) * TN : (2 - d) * TN])
        send(NEAR, d, 0)
        carry[d] = v[:, d * TN : (d + 1) * TN]
    wait(d_loads[3], "d3")
    yacc[...] = jnp.dot(hid[...], wd[3], preferred_element_type=F32)

    def got(kind, d, p):
        with jax.named_scope(f"got{kind}{d}{p}"):
            hop(kind, d, p).wait_recv()
        return recv[(kind * 2 + d) * 2 + p].astype(F32)

    for p in (0, 1):
        for d in (RIGHT, LEFT):
            put(CARRY, d, p, carry[d, part(p), :] + got(FAR, d, p))
            send(CARRY, d, p)
        if p == 0:
            for d in (RIGHT, LEFT):
                send(NEAR, d, 1)

    def place(k, owner, h, width):
        return pl.ds(pl.multiple_of(k * cols + owner * block + h * TN, TN), width)

    def share(p, d, h):
        move = remote(yb.at[p, :, pl.ds(h * TN, TN)], y_ref.at[:, place(core, t, h, TN)],
                      ag_send.at[p, d, h], ag_recv.at[d, h, core], dev(to[d], base + p))
        move.start()
        sends.append(move)

    for p in (0, 1):
        for d in (RIGHT, LEFT):
            at = slice(d * TN, (d + 1) * TN)
            yb[p, :, at] = (yacc[part(p), at] + got(CARRY, d, p) + got(NEAR, 1 - d, p)).astype(BF16)
            share(p, d, d)
        for d in (RIGHT, LEFT):
            share(p, d, 1 - d)

        @pl.when(core == p)
        def _():
            y_ref[:, place(core, t, 0, block)] = yb[p]

        @pl.when(core != p)
        def _():
            remote(yb.at[p], y_ref.at[:, place(core, t, 0, block)], own_send, own_recv, dev(t, other)).start()

    def landed(d, h, k):
        at = place(k, (left, right)[d], h, TN)
        with jax.named_scope(f"land{d}{h}{k}"):
            remote(y_ref.at[:, at], y_ref.at[:, at], ag_send.at[0, d, h], ag_recv.at[d, h, k], dev(to[d], g)).wait_recv()
        return at

    for k in (0, 1):
        for d in (RIGHT, LEFT):
            at = landed(d, d, k)
            move = remote(y_ref.at[:, at], y_ref.at[:, at], fw_send.at[d, k], fw_recv.at[d, k], dev(to[d], g))
            move.start()
            sends.append(move)
    for k in (0, 1):
        for d in (RIGHT, LEFT):
            landed(d, 1 - d, k)
    at = place(1 - core, t, 0, block)
    sib = remote(yb.at[0], y_ref.at[:, at], own_send, own_recv, dev(t, other))
    sib.wait_recv()
    for k in (0, 1):
        for d in (RIGHT, LEFT):
            at = place(k, far, d, TN)
            with jax.named_scope(f"fw{d}{k}"):
                remote(y_ref.at[:, at], y_ref.at[:, at], fw_send.at[d, k], fw_recv.at[d, k], dev(to[d], g)).wait_recv()
    sib.wait_send()
    for move in x_moves + h_moves + sends:
        move.wait_send()


def solution(mesh):
    n = mesh.shape["tp"]

    def step(x, w_gate, w_up, w_down):
        rows, depth = x.shape
        hidden, out = w_down.shape
        half, cols = hidden // 2, out // 2
        steps = half // TK
        DMA = pltpu.SemaphoreType.DMA
        any_spec = pl.BlockSpec(memory_space=pl.ANY)
        return pl.pallas_call(
            functools.partial(kernel, n),
            out_shape=pltpu.VMEM((rows, out), BF16),
            in_specs=[any_spec] * 4,
            out_specs=pl.BlockSpec(memory_space=pltpu.VMEM),
            scratch_shapes=[
                pltpu.VMEM((2 * rows, depth), BF16),
                pltpu.VMEM((steps, depth, 2 * TK), BF16),
                pltpu.VMEM((n, hidden, cols // n), BF16),
                pltpu.VMEM((2, 2 * rows, 2 * TK), F32),
                pltpu.VMEM((2 * rows, hidden), BF16),
                pltpu.VMEM((2 * rows, cols // n), F32),
                pltpu.VMEM((2, 2 * rows, TN), F32),
                pltpu.VMEM((12, rows, TN), BF16),
                pltpu.VMEM((12, rows, TN), BF16),
                pltpu.VMEM((2, rows, 2 * TN), BF16),
                DMA((XP,)), DMA((XP,)), DMA((XP,)), DMA((steps, 2)), DMA((n, 2)), DMA((steps,)), DMA((steps,)),
                DMA((12,)), DMA((12,)), DMA((2, 2, 2)), DMA((2, 2, 2)), DMA((2, 2)), DMA((2, 2)), DMA, DMA,
            ],
            compiler_params=pltpu.CompilerParams(
                collective_id=0, has_side_effects=True, vmem_limit_bytes=56 * 1024 * 1024
            ),
        )(x, w_gate, w_up, w_down)

    return jax.shard_map(
        step,
        mesh=mesh,
        in_specs=(P("dp", None), P(None, "tp"), P(None, "tp"), P("tp", None)),
        out_specs=P("dp", None),
        check_vma=False,
    )
```

```python
import functools

import jax
import jax.numpy as jnp
from jax import lax
from jax.experimental import pallas as pl
from jax.experimental.pallas import tpu as pltpu
from jax.sharding import PartitionSpec as P

MESH = pl.DeviceIdType.MESH
BF16 = jnp.bfloat16
F32 = jnp.float32
T = 256
Q = 4
FAR, NEAR, CARRY = 0, 1, 2
RIGHT, LEFT = 0, 1
OWN, HIS = 0, 1


def kernel(
    n, x_hbm, wg_hbm, wu_hbm, wd_hbm, y_ref,
    xv, wgu, wd, gacc, hid, far_sum, ysum, carry, stage, far_in, near_in, yb,
    x_sem, w_sem, d_sem, sent, x_recv, h_recv, far_recv, near_recv, pass_recv, end_recv, met,
):
    t = lax.axis_index("tp")
    g = lax.axis_index("dp")
    core = lax.rem(g, 2)
    other = g + 1 - 2 * core
    right, left = lax.rem(t + 1, n), lax.rem(t + n - 1, n)
    far = lax.rem(t + 2, n)
    rows, depth = x_hbm.shape
    half = wg_hbm.shape[1] // 2
    steps = half // T
    cols = wd_hbm.shape[1] // 2
    block = cols // n
    to = (right, left)

    def dev(tp, dp):
        return {"tp": tp, "dp": dp}

    def remote(src, dst, send, rcv, device):
        return pltpu.make_async_remote_copy(
            src_ref=src, dst_ref=dst, send_sem=send, recv_sem=rcv,
            device_id=device, device_id_type=MESH,
        )

    def start(copies):
        for copy in copies:
            copy.start(priority=1)

    def wait(copies, name):
        with jax.named_scope(name):
            for copy in copies:
                copy.wait()

    deep = [pl.ds(k * (depth // Q), depth // Q) for k in range(Q)]
    x_loads = [pltpu.make_async_copy(x_hbm.at[:, at], xv.at[OWN, :, at], x_sem.at[k]) for k, at in enumerate(deep)]
    for copy in x_loads:
        copy.start()
    upper, lower, full = pl.ds(0, depth // 2), pl.ds(depth // 2, depth // 2), pl.ds(0, depth)
    parts = [(j, at) for j in range(steps) for at in ((upper, lower) if j == 1 else (full,))]
    for i, (j, at) in enumerate(parts):
        start([pltpu.make_async_copy(
            w.at[at, pl.ds(pl.multiple_of(core * half + j * T, T), T)], wgu.at[j, at, pl.ds(q * T, T)], w_sem.at[i])
            for q, w in enumerate((wg_hbm, wu_hbm))])

    def load(i):
        j, at = parts[i]
        wait([pltpu.make_async_copy(wg_hbm.at[at, pl.ds(0, 2 * T)], wgu.at[j, at, :], w_sem.at[i])], f"w{i}")

    def take(sem, width):
        at = pl.ds(0, width)
        pltpu.make_async_copy(x_hbm.at[:, at], xv.at[OWN, :, at], sem).wait()

    d_loads = []
    for s, owner in enumerate((far, right, left, t)):
        at = pl.ds(pl.multiple_of(core * cols + owner * block, block), block)
        d_loads.append([
            pltpu.make_async_copy(
                wd_hbm.at[pl.ds(pl.multiple_of(c * half, half), half), at],
                wd.at[s, pl.ds(i * half, half), :], d_sem.at[s])
            for i, c in enumerate((core, 1 - core))])

    def load_down(s):
        wait([pltpu.make_async_copy(wd_hbm.at[:, pl.ds(0, block)], wd.at[s], d_sem.at[s])], f"d{s}")

    barrier = pltpu.get_barrier_semaphore()

    def signal(sem, device):
        pl.semaphore_signal(sem, inc=1, device_id=device, device_id_type=MESH)

    @pl.when(core == 0)
    def _():
        signal(barrier, dev(t, other))

    @pl.when(core == 1)
    def _():
        pl.semaphore_wait(barrier, 1)
        signal(met, dev(t, other))


    @pl.when(core == 0)
    def _():
        pl.semaphore_wait(met, 1)
        for a in to:
            signal(barrier, dev(a, g))

    for k, at in enumerate(deep):
        wait([x_loads[k]], "xl")
        remote(xv.at[OWN, :, at], xv.at[HIS, :, at], sent.at[0], x_recv, dev(t, other)).start()

    def dot(a, b):
        return jnp.dot(a, b, preferred_element_type=F32)

    def gate_up(j, rs, at=slice(None)):
        return dot(xv[rs, :, at], wgu[j, at, :])


    last = steps - 1

    def activate(j, rs, a):
        hid[rs, :, j * T : (j + 1) * T] = (jax.nn.gelu(a[:, :T]) * a[:, T:]).astype(BF16)

    def give(j, rs):
        remote(
            hid.at[rs, :, pl.ds(j * T, T)], hid.at[1 - rs, :, pl.ds(half + j * T, T)],
            sent.at[1], h_recv.at[1 - rs, j // last], dev(t, other)).start()

    both = (OWN, HIS)
    load(0)
    gacc[0] = gate_up(0, OWN)
    load(1)
    gacc[1] = gate_up(1, OWN, slice(0, depth // 2))
    load(2)
    with jax.named_scope("x"):
        take(x_recv, depth)
    activate(0, OWN, gacc[0])
    activate(0, HIS, gate_up(0, HIS))
    activate(1, OWN, gacc[1] + gate_up(1, OWN, slice(depth // 2, depth)))
    activate(1, HIS, gate_up(1, HIS))
    for j in (0, 1):
        for rs in both:
            give(j, rs)
    for j in range(2, last):
        load(j + 1)
        start(d_loads[j - 2])
        a = dot(xv[...].reshape(2 * rows, depth), wgu[j])
        for rs in both:
            activate(j, rs, a[rs * rows : (rs + 1) * rows])
        for rs in both:
            give(j, rs)
        if j == 2:

            @pl.when(core == 0)
            def _():
                pl.semaphore_wait(barrier, 2)
                signal(met, dev(t, other))

    load(last + 1)
    for s in range(last - 2, n):
        start(d_loads[s])
    for rs in (HIS, OWN):
        activate(last, rs, gate_up(last, rs))
        give(last, rs)

    @pl.when(core == 1)
    def _():
        pl.semaphore_wait(met, 1)

    def hop(kind, d, rs):
        dst, sem = {
            FAR: (far_in.at[d * 2 + rs], far_recv.at[d * 2 + rs]),
            CARRY: (near_in.at[d * 2 + rs, 0], near_recv.at[d * 2 + rs]),
            NEAR: (near_in.at[(1 - d) * 2 + rs, 1], near_recv.at[(1 - d) * 2 + rs]),
        }[kind]
        return remote(stage.at[(kind * 2 + d) * 2 + rs], dst, sent.at[2], sem, dev(to[d], g))

    def put(kind, d, rs, v):
        stage[(kind * 2 + d) * 2 + rs] = v.astype(BF16)

    def send(kind, d, rs):
        hop(kind, d, rs).start()

    load_down(0)
    most = 2 * half - T
    for rs in both:
        with jax.named_scope(f"h{rs}"):
            take(h_recv.at[rs, 0], last * T)
        far_sum[rs] = dot(hid[rs, :, :most], wd[0, :most, :])
        with jax.named_scope(f"hl{rs}"):
            take(h_recv.at[rs, 1], T)
        v = far_sum[rs] + dot(hid[rs, :, most:], wd[0, most:, :])
        for d in (RIGHT, LEFT):
            put(FAR, d, rs, v[:, d * T : (d + 1) * T])
        for d in (RIGHT, LEFT):
            send(FAR, d, rs)

    def down(s):
        return dot(hid[...].reshape(2 * rows, 2 * half), wd[s])

    for d in (RIGHT, LEFT):
        load_down(1 + d)
        v = down(1 + d)
        for rs in both:
            put(NEAR, d, rs, v[rs * rows : (rs + 1) * rows, (1 - d) * T : (2 - d) * T])
            carry[d, rs] = v[rs * rows : (rs + 1) * rows, d * T : (d + 1) * T]
        send(NEAR, d, OWN)
    load_down(3)
    v = down(3)
    for rs in both:
        ysum[rs] = v[rs * rows : (rs + 1) * rows]

    for rs in both:
        for d in (RIGHT, LEFT):
            with jax.named_scope(f"far{d}{rs}"):
                take(far_recv.at[d * 2 + rs], T)
            put(CARRY, d, rs, carry[d, rs] + far_in[d * 2 + rs].astype(F32))
            send(CARRY, d, rs)
        if rs == OWN:
            for d in (RIGHT, LEFT):
                send(NEAR, d, HIS)

    def place(k, owner, h, width):
        return pl.ds(pl.multiple_of(k * cols + owner * block + h * T, T), width)

    def share(rs, d, h):
        at = place(core, t, h, T)
        remote(yb.at[rs, :, pl.ds(h * T, T)], y_ref.at[:, at], sent.at[3],
               pass_recv.at[rs, d] if d == h else end_recv, dev(to[d], (g, other)[rs])).start()

    mine = place(core, t, 0, block)
    for rs in both:
        for d in (RIGHT, LEFT):
            i = d * 2 + rs
            with jax.named_scope(f"near{d}{rs}"):
                take(near_recv.at[i], 2 * T)
            yb[rs, :, d * T : (d + 1) * T] = (
                ysum[rs, :, d * T : (d + 1) * T] + near_in[i, 0].astype(F32) + near_in[i, 1].astype(F32)).astype(BF16)
            share(rs, d, d)
        for d in (RIGHT, LEFT):
            share(rs, d, 1 - d)
        if rs == OWN:
            y_ref[:, mine] = yb[OWN]
        else:
            remote(yb.at[HIS], y_ref.at[:, mine], sent.at[3], end_recv, dev(t, other)).start()

    for rs in both:
        for d in (RIGHT, LEFT):
            with jax.named_scope(f"pass{d}{rs}"):
                take(pass_recv.at[rs, d], T)
            at = place((core, 1 - core)[rs], (left, right)[d], d, T)
            remote(y_ref.at[:, at], y_ref.at[:, at], sent.at[4], end_recv, dev(to[d], g)).start()
    with jax.named_scope("end"):
        take(end_recv, 8 * T + block)
    with jax.named_scope("sends"):
        for i, width in enumerate((depth, 2 * half, 12 * T, 8 * T + block, 4 * T)):
            take(sent.at[i], width)


def solution(mesh):
    n = mesh.shape["tp"]

    def step(x, w_gate, w_up, w_down):
        rows, depth = x.shape
        hidden, out = w_down.shape
        steps, block = hidden // 2 // T, out // 2 // n
        DMA = pltpu.SemaphoreType.DMA
        hbm = pl.BlockSpec(memory_space=pl.ANY)
        return pl.pallas_call(
            functools.partial(kernel, n),
            out_shape=pltpu.VMEM((rows, out), BF16),
            in_specs=[hbm] * 4,
            out_specs=pl.BlockSpec(memory_space=pltpu.VMEM),
            scratch_shapes=[
                pltpu.VMEM((2, rows, depth), BF16),
                pltpu.VMEM((steps, depth, 2 * T), BF16),
                pltpu.VMEM((n, hidden, block), BF16),
                pltpu.VMEM((2, rows, 2 * T), F32),
                pltpu.VMEM((2, rows, hidden), BF16),
                pltpu.VMEM((2, rows, block), F32),
                pltpu.VMEM((2, rows, block), F32),
                pltpu.VMEM((2, 2, rows, T), F32),
                pltpu.VMEM((12, rows, T), BF16),
                pltpu.VMEM((4, rows, T), BF16),
                pltpu.VMEM((4, 2, rows, T), BF16),
                pltpu.VMEM((2, rows, block), BF16),
                DMA((Q,)), DMA((steps + 1,)), DMA((n,)), DMA((5,)),
                DMA, DMA((2, 2)), DMA((4,)), DMA((4,)), DMA((2, 2)), DMA, pltpu.SemaphoreType.REGULAR,
            ],
            compiler_params=pltpu.CompilerParams(
                collective_id=0, has_side_effects=True, vmem_limit_bytes=56 * 1024 * 1024
            ),
        )(x, w_gate, w_up, w_down)

    return jax.shard_map(
        step,
        mesh=mesh,
        in_specs=(P("dp", None), P(None, "tp"), P(None, "tp"), P("tp", None)),
        out_specs=P("dp", None),
        check_vma=False,
    )
```

```python
import functools

import jax
import jax.numpy as jnp
from jax import lax
from jax.experimental import pallas as pl
from jax.experimental.pallas import tpu as pltpu
from jax.sharding import PartitionSpec as P

MESH = pl.DeviceIdType.MESH
BF16 = jnp.bfloat16
F32 = jnp.float32
T = 256
Q = 4
FAR, NEAR, CARRY = 0, 1, 2
RIGHT, LEFT = 0, 1


def kernel(n, *refs):
    DMA = pltpu.SemaphoreType.DMA
    steps = refs[1].shape[1] // 2 // T
    pl.run_scoped(functools.partial(body, n, *refs), DMA((Q,)), DMA((steps + 1,)), DMA((n,)), DMA((5,)))


def body(
    n, x_hbm, wg_hbm, wu_hbm, wd_hbm, y_ref,
    xv, wgu, wd, gacc, hid, far_sum, ysum, carry, stage, far_in, near_in, yb,
    x_recv, h_recv, far_recv, near_recv, pass_recv, end_recv, met,
    x_sem, w_sem, d_sem, sent,
):
    t = lax.axis_index("tp")
    g = lax.axis_index("dp")
    core = lax.rem(g, 2)
    groups = (g - core, g - core + 1)
    other = g + 1 - 2 * core
    right, left = lax.rem(t + 1, n), lax.rem(t + n - 1, n)
    far = lax.rem(t + 2, n)
    rows, depth = x_hbm.shape
    half = wg_hbm.shape[1] // 2
    steps = half // T
    cols = wd_hbm.shape[1] // 2
    block = cols // n
    to = (right, left)

    def dev(tp, dp):
        return {"tp": tp, "dp": dp}

    def remote(src, dst, send, rcv, device):
        return pltpu.make_async_remote_copy(
            src_ref=src, dst_ref=dst, send_sem=send, recv_sem=rcv,
            device_id=device, device_id_type=MESH,
        )

    def start(copies):
        for copy in copies:
            copy.start(priority=1)

    def wait(copies, name):
        with jax.named_scope(name):
            for copy in copies:
                copy.wait()

    deep = [pl.ds(k * (depth // Q), depth // Q) for k in range(Q)]
    x_loads = [pltpu.make_async_copy(x_hbm.at[:, at], xv.at[core, :, at], x_sem.at[k]) for k, at in enumerate(deep)]
    for copy in x_loads:
        copy.start()
    upper, lower, full = pl.ds(0, depth // 2), pl.ds(depth // 2, depth // 2), pl.ds(0, depth)
    parts = [(j, at) for j in range(steps) for at in ((upper, lower) if j == 1 else (full,))]
    for i, (j, at) in enumerate(parts):
        start([pltpu.make_async_copy(
            w.at[at, pl.ds(pl.multiple_of(core * half + j * T, T), T)], wgu.at[j, at, pl.ds(q * T, T)], w_sem.at[i])
            for q, w in enumerate((wg_hbm, wu_hbm))])

    def load(i):
        j, at = parts[i]
        wait([pltpu.make_async_copy(wg_hbm.at[at, pl.ds(0, 2 * T)], wgu.at[j, at, :], w_sem.at[i])], f"w{i}")

    def take(sem, width):
        at = pl.ds(0, width)
        pltpu.make_async_copy(x_hbm.at[:, at], xv.at[0, :, at], sem).wait()

    d_loads = []
    for s, owner in enumerate((far, right, left, t)):
        at = pl.ds(pl.multiple_of(core * cols + owner * block, block), block)
        d_loads.append([
            pltpu.make_async_copy(
                wd_hbm.at[pl.ds(pl.multiple_of(c * half, half), half), at],
                wd.at[s, pl.ds(i * half, half), :], d_sem.at[s])
            for i, c in enumerate((core, 1 - core))])

    def load_down(s):
        wait([pltpu.make_async_copy(wd_hbm.at[:, pl.ds(0, block)], wd.at[s], d_sem.at[s])], f"d{s}")

    barrier = pltpu.get_barrier_semaphore()

    def signal(sem, device):
        pl.semaphore_signal(sem, inc=1, device_id=device, device_id_type=MESH)

    @pl.when(core == 0)
    def _():
        signal(barrier, dev(t, other))

    @pl.when(core == 1)
    def _():
        pl.semaphore_wait(barrier, 1)
        signal(met, dev(t, other))


    @pl.when(core == 0)
    def _():
        pl.semaphore_wait(met, 1)
        for a in to:
            signal(barrier, dev(a, g))

    for k, at in enumerate(deep):
        wait([x_loads[k]], "xl")
        remote(xv.at[core, :, at], xv.at[core, :, at], sent.at[0], x_recv, dev(t, other)).start()

    def dot(a, b):
        return jnp.dot(a, b, preferred_element_type=F32)

    def gate_up(j, p, at=slice(None)):
        return dot(xv[p, :, at], wgu[j, at, :])

    last = steps - 1

    def activate(j, p, a):
        hid[p, :, j * T : (j + 1) * T] = (jax.nn.gelu(a[:, :T]) * a[:, T:]).astype(BF16)

    def give(j, p):
        remote(
            hid.at[p, :, pl.ds(j * T, T)], hid.at[p, :, pl.ds(half + j * T, T)],
            sent.at[1], h_recv.at[p, j // last], dev(t, other)).start()

    both = (0, 1)
    load(0)
    gacc[0] = gate_up(0, core)
    load(1)
    gacc[1] = gate_up(1, core, slice(0, depth // 2))
    load(2)
    with jax.named_scope("x"):
        take(x_recv, depth)
    activate(0, core, gacc[0])
    activate(0, 1 - core, gate_up(0, 1 - core))
    activate(1, core, gacc[1] + gate_up(1, core, slice(depth // 2, depth)))
    activate(1, 1 - core, gate_up(1, 1 - core))
    for j in (0, 1):
        for p in both:
            give(j, p)
    for j in range(2, last - 1):
        load(j + 1)
        start(d_loads[j - 2])
        a = dot(xv[...].reshape(2 * rows, depth), wgu[j])
        for p in both:
            activate(j, p, a[p * rows : (p + 1) * rows])
        for p in both:
            give(j, p)

    @pl.when(core == 0)
    def _():
        pl.semaphore_wait(barrier, 2)
        signal(met, dev(t, other))

    load(last)
    for s in range(last - 3, n):
        start(d_loads[s])
    activate(last - 1, 0, gate_up(last - 1, 0))
    give(last - 1, 0)
    load(last + 1)
    activate(last, 0, gate_up(last, 0))
    give(last, 0)
    activate(last - 1, 1, gate_up(last - 1, 1))
    give(last - 1, 1)

    @pl.when(core == 1)
    def _():
        pl.semaphore_wait(met, 1)

    def hop(kind, d, rs):
        dst, sem = {
            FAR: (far_in.at[d * 2 + rs], far_recv.at[d * 2 + rs]),
            CARRY: (near_in.at[d * 2 + rs, 0], near_recv.at[d * 2 + rs]),
            NEAR: (near_in.at[(1 - d) * 2 + rs, 1], near_recv.at[(1 - d) * 2 + rs]),
        }[kind]
        return remote(stage.at[(kind * 2 + d) * 2 + rs], dst, sent.at[2], sem, dev(to[d], g))

    def put(kind, d, rs, v):
        stage[(kind * 2 + d) * 2 + rs] = v.astype(BF16)

    def send(kind, d, rs):
        hop(kind, d, rs).start()

    most = 2 * half - T

    def far_block(p):
        with jax.named_scope(f"h{p}"):
            take(h_recv.at[p, 0], last * T)
        far_sum[p] = dot(hid[p, :, :most], wd[0, :most, :])
        with jax.named_scope(f"hl{p}"):
            take(h_recv.at[p, 1], T)
        v = far_sum[p] + dot(hid[p, :, most:], wd[0, most:, :])
        for d in (RIGHT, LEFT):
            put(FAR, d, p, v[:, d * T : (d + 1) * T])
        for d in (RIGHT, LEFT):
            send(FAR, d, p)

    def down(s, p, d):
        return dot(hid[p], wd[s, :, d * T : (d + 1) * T])

    load_down(0)
    far_block(0)
    activate(last, 1, gate_up(last, 1))
    give(last, 1)
    load_down(1)
    load_down(2)
    for d in (RIGHT, LEFT):
        put(NEAR, d, 0, down(1 + d, 0, 1 - d))
    for d in (RIGHT, LEFT):
        send(NEAR, d, 0)
    far_block(1)
    for d in (RIGHT, LEFT):
        carry[d, 0] = down(1 + d, 0, d)
        carry[d, 1] = down(1 + d, 1, d)
        put(NEAR, d, 1, down(1 + d, 1, 1 - d))
    for p in both:
        for d in (RIGHT, LEFT):
            with jax.named_scope(f"far{d}{p}"):
                take(far_recv.at[d * 2 + p], T)
            put(CARRY, d, p, carry[d, p] + far_in[d * 2 + p].astype(F32))
            send(CARRY, d, p)
        if p == 0:
            for d in (RIGHT, LEFT):
                send(NEAR, d, 1)
            load_down(3)
            v = dot(hid[...].reshape(2 * rows, 2 * half), wd[3])
            for r in both:
                ysum[r] = v[r * rows : (r + 1) * rows]

    def place(k, owner, h, width):
        return pl.ds(pl.multiple_of(k * cols + owner * block + h * T, T), width)

    def share(p, d, h):
        at = place(core, t, h, T)
        remote(yb.at[p, :, pl.ds(h * T, T)], y_ref.at[:, at], sent.at[3],
               pass_recv.at[core, d] if d == h else end_recv, dev(to[d], groups[p])).start()

    mine = place(core, t, 0, block)
    for p in both:
        for d in (RIGHT, LEFT):
            i = d * 2 + p
            with jax.named_scope(f"near{d}{p}"):
                take(near_recv.at[i], 2 * T)
            yb[p, :, d * T : (d + 1) * T] = (
                ysum[p, :, d * T : (d + 1) * T] + near_in[i, 0].astype(F32) + near_in[i, 1].astype(F32)).astype(BF16)
            share(p, d, d)
        for d in (RIGHT, LEFT):
            share(p, d, 1 - d)
    y_ref[:, mine] = yb[core]
    remote(yb.at[1 - core], y_ref.at[:, mine], sent.at[3], end_recv, dev(t, other)).start()

    for p in both:
        for d in (RIGHT, LEFT):
            with jax.named_scope(f"pass{d}{p}"):
                take(pass_recv.at[p, d], T)
            at = place(p, (left, right)[d], d, T)
            remote(y_ref.at[:, at], y_ref.at[:, at], sent.at[4], end_recv, dev(to[d], g)).start()
    with jax.named_scope("end"):
        take(end_recv, 8 * T + block)
    with jax.named_scope("sends"):
        for i, width in enumerate((depth, 2 * half, 12 * T, 8 * T + block, 4 * T)):
            take(sent.at[i], width)


def solution(mesh):
    n = mesh.shape["tp"]

    def step(x, w_gate, w_up, w_down):
        rows, depth = x.shape
        hidden, out = w_down.shape
        steps, block = hidden // 2 // T, out // 2 // n
        DMA = pltpu.SemaphoreType.DMA
        hbm = pl.BlockSpec(memory_space=pl.ANY)
        return pl.pallas_call(
            functools.partial(kernel, n),
            out_shape=pltpu.VMEM((rows, out), BF16),
            in_specs=[hbm] * 4,
            out_specs=pl.BlockSpec(memory_space=pltpu.VMEM),
            scratch_shapes=[
                pltpu.VMEM((2, rows, depth), BF16),
                pltpu.VMEM((steps, depth, 2 * T), BF16),
                pltpu.VMEM((n, hidden, block), BF16),
                pltpu.VMEM((2, rows, 2 * T), F32),
                pltpu.VMEM((2, rows, hidden), BF16),
                pltpu.VMEM((2, rows, block), F32),
                pltpu.VMEM((2, rows, block), F32),
                pltpu.VMEM((2, 2, rows, T), F32),
                pltpu.VMEM((12, rows, T), BF16),
                pltpu.VMEM((4, rows, T), BF16),
                pltpu.VMEM((4, 2, rows, T), BF16),
                pltpu.VMEM((2, rows, block), BF16),
                DMA, DMA((2, 2)), DMA((4,)), DMA((4,)), DMA((2, 2)), DMA, pltpu.SemaphoreType.REGULAR,
            ],
            compiler_params=pltpu.CompilerParams(
                collective_id=0, has_side_effects=True, vmem_limit_bytes=56 * 1024 * 1024
            ),
        )(x, w_gate, w_up, w_down)

    return jax.shard_map(
        step,
        mesh=mesh,
        in_specs=(P("dp", None), P(None, "tp"), P(None, "tp"), P("tp", None)),
        out_specs=P("dp", None),
        check_vma=False,
    )
```

```python
import functools

import jax
import jax.numpy as jnp
from jax import lax
from jax.experimental import pallas as pl
from jax.experimental.pallas import tpu as pltpu
from jax.sharding import PartitionSpec as P

MESH = pl.DeviceIdType.MESH
BF16 = jnp.bfloat16
F32 = jnp.float32
T = 256
Q = 4
FAR, NEAR, CARRY = 0, 1, 2
RIGHT, LEFT = 0, 1


def kernel(n, *refs):
    DMA = pltpu.SemaphoreType.DMA
    steps = refs[1].shape[1] // 2 // T
    pl.run_scoped(
        functools.partial(body, n, *refs),
        DMA((Q,)), DMA((steps + 1,)), DMA((n,)), DMA((5,)),
        DMA, DMA((2, 2)), DMA((4,)), DMA((4,)), DMA((2, 2)), DMA,
    )


def body(
    n, x_hbm, wg_hbm, wu_hbm, wd_hbm, y_ref,
    xv, wgu, wd, gacc, hid, far_sum, ysum, carry, stage, far_in, near_in, yb,
    met, x_sem, w_sem, d_sem, sent, x_recv, h_recv, far_recv, near_recv, pass_recv, end_recv,
):
    t = lax.axis_index("tp")
    g = lax.axis_index("dp")
    core = lax.rem(g, 2)
    groups = (g - core, g - core + 1)
    other = g + 1 - 2 * core
    right, left = lax.rem(t + 1, n), lax.rem(t + n - 1, n)
    far = lax.rem(t + 2, n)
    rows, depth = x_hbm.shape
    half = wg_hbm.shape[1] // 2
    steps = half // T
    cols = wd_hbm.shape[1] // 2
    block = cols // n
    to = (right, left)

    def dev(tp, dp):
        return {"tp": tp, "dp": dp}

    def remote(src, dst, send, rcv, device):
        return pltpu.make_async_remote_copy(
            src_ref=src, dst_ref=dst, send_sem=send, recv_sem=rcv,
            device_id=device, device_id_type=MESH,
        )

    def start(copies):
        for copy in copies:
            copy.start(priority=1)

    def wait(copies, name):
        with jax.named_scope(name):
            for copy in copies:
                copy.wait()

    deep = [pl.ds(k * (depth // Q), depth // Q) for k in range(Q)]
    x_loads = [pltpu.make_async_copy(x_hbm.at[:, at], xv.at[core, :, at], x_sem.at[k]) for k, at in enumerate(deep)]
    for copy in x_loads:
        copy.start()
    upper, lower, full = pl.ds(0, depth // 2), pl.ds(depth // 2, depth // 2), pl.ds(0, depth)
    parts = [(j, at) for j in range(steps) for at in ((upper, lower) if j == 1 else (full,))]
    for i, (j, at) in enumerate(parts):
        start([pltpu.make_async_copy(
            w.at[at, pl.ds(pl.multiple_of(core * half + j * T, T), T)], wgu.at[j, at, pl.ds(q * T, T)], w_sem.at[i])
            for q, w in enumerate((wg_hbm, wu_hbm))])

    def load(i):
        j, at = parts[i]
        wait([pltpu.make_async_copy(wg_hbm.at[at, pl.ds(0, 2 * T)], wgu.at[j, at, :], w_sem.at[i])], f"w{i}")

    def take(sem, width):
        at = pl.ds(0, width)
        pltpu.make_async_copy(x_hbm.at[:, at], xv.at[0, :, at], sem).wait()

    d_loads = []
    for s, owner in enumerate((far, right, left, t)):
        at = pl.ds(pl.multiple_of(core * cols + owner * block, block), block)
        d_loads.append([
            pltpu.make_async_copy(
                wd_hbm.at[pl.ds(pl.multiple_of(c * half, half), half), at],
                wd.at[s, pl.ds(i * half, half), :], d_sem.at[s])
            for i, c in enumerate((core, 1 - core))])

    def load_down(s):
        wait([pltpu.make_async_copy(wd_hbm.at[:, pl.ds(0, block)], wd.at[s], d_sem.at[s])], f"d{s}")

    barrier = pltpu.get_barrier_semaphore()

    def signal(sem, device):
        pl.semaphore_signal(sem, inc=1, device_id=device, device_id_type=MESH)

    @pl.when(core == 0)
    def _():
        signal(barrier, dev(t, other))

    @pl.when(core == 1)
    def _():
        pl.semaphore_wait(barrier, 1)
        signal(met, dev(t, other))


    @pl.when(core == 0)
    def _():
        pl.semaphore_wait(met, 1)
        for a in to:
            signal(barrier, dev(a, g))

    for k, at in enumerate(deep):
        wait([x_loads[k]], "xl")
        remote(xv.at[core, :, at], xv.at[core, :, at], sent.at[0], x_recv, dev(t, other)).start()

    def dot(a, b):
        return jnp.dot(a, b, preferred_element_type=F32)

    def gate_up(j, p, at=slice(None)):
        return dot(xv[p, :, at], wgu[j, at, :])

    last = steps - 1

    def activate(j, p, a):
        hid[p, :, j * T : (j + 1) * T] = (jax.nn.gelu(a[:, :T]) * a[:, T:]).astype(BF16)

    def give(j, p):
        remote(
            hid.at[p, :, pl.ds(j * T, T)], hid.at[p, :, pl.ds(half + j * T, T)],
            sent.at[1], h_recv.at[p, j // last], dev(t, other)).start()

    both = (0, 1)
    load(0)
    gacc[0] = gate_up(0, core)
    load(1)
    gacc[1] = gate_up(1, core, slice(0, depth // 2))
    load(2)
    with jax.named_scope("x"):
        take(x_recv, depth)
    activate(0, core, gacc[0])
    activate(0, 1 - core, gate_up(0, 1 - core))
    activate(1, core, gacc[1] + gate_up(1, core, slice(depth // 2, depth)))
    activate(1, 1 - core, gate_up(1, 1 - core))
    for j in (0, 1):
        for p in both:
            give(j, p)
    for j in range(2, last - 1):
        load(j + 1)
        start(d_loads[j - 2])
        a = dot(xv[...].reshape(2 * rows, depth), wgu[j])
        for p in both:
            activate(j, p, a[p * rows : (p + 1) * rows])
        for p in both:
            give(j, p)

    @pl.when(core == 0)
    def _():
        pl.semaphore_wait(barrier, 2)
        signal(met, dev(t, other))

    load(last)
    for s in range(last - 3, n):
        start(d_loads[s])
    activate(last - 1, 0, gate_up(last - 1, 0))
    give(last - 1, 0)
    load(last + 1)
    activate(last, 0, gate_up(last, 0))
    give(last, 0)
    activate(last - 1, 1, gate_up(last - 1, 1))
    give(last - 1, 1)

    @pl.when(core == 1)
    def _():
        pl.semaphore_wait(met, 1)

    def hop(kind, d, rs):
        dst, sem = {
            FAR: (far_in.at[d * 2 + rs], far_recv.at[d * 2 + rs]),
            CARRY: (near_in.at[d * 2 + rs, 0], near_recv.at[d * 2 + rs]),
            NEAR: (near_in.at[(1 - d) * 2 + rs, 1], near_recv.at[(1 - d) * 2 + rs]),
        }[kind]
        return remote(stage.at[(kind * 2 + d) * 2 + rs], dst, sent.at[2], sem, dev(to[d], g))

    def put(kind, d, rs, v):
        stage[(kind * 2 + d) * 2 + rs] = v.astype(BF16)

    def send(kind, d, rs):
        hop(kind, d, rs).start()

    most = 2 * half - T

    def far_block(p):
        with jax.named_scope(f"h{p}"):
            take(h_recv.at[p, 0], last * T)
        far_sum[p] = dot(hid[p, :, :most], wd[0, :most, :])
        with jax.named_scope(f"hl{p}"):
            take(h_recv.at[p, 1], T)
        v = far_sum[p] + dot(hid[p, :, most:], wd[0, most:, :])
        for d in (RIGHT, LEFT):
            put(FAR, d, p, v[:, d * T : (d + 1) * T])
        for d in (RIGHT, LEFT):
            send(FAR, d, p)

    def down(s, p, d):
        return dot(hid[p], wd[s, :, d * T : (d + 1) * T])

    load_down(0)
    far_block(0)
    activate(last, 1, gate_up(last, 1))
    give(last, 1)
    load_down(1)
    load_down(2)
    for d in (RIGHT, LEFT):
        put(NEAR, d, 0, down(1 + d, 0, 1 - d))
    for d in (RIGHT, LEFT):
        send(NEAR, d, 0)
    far_block(1)
    for d in (RIGHT, LEFT):
        carry[d, 0] = down(1 + d, 0, d)
        carry[d, 1] = down(1 + d, 1, d)
        put(NEAR, d, 1, down(1 + d, 1, 1 - d))
    for p in both:
        for d in (RIGHT, LEFT):
            with jax.named_scope(f"far{d}{p}"):
                take(far_recv.at[d * 2 + p], T)
            put(CARRY, d, p, carry[d, p] + far_in[d * 2 + p].astype(F32))
            send(CARRY, d, p)
        if p == 0:
            for d in (RIGHT, LEFT):
                send(NEAR, d, 1)
            load_down(3)
            v = dot(hid[...].reshape(2 * rows, 2 * half), wd[3])
            for r in both:
                ysum[r] = v[r * rows : (r + 1) * rows]

    def place(k, owner, h, width):
        return pl.ds(pl.multiple_of(k * cols + owner * block + h * T, T), width)

    def share(p, d, h):
        at = place(core, t, h, T)
        remote(yb.at[p, :, pl.ds(h * T, T)], y_ref.at[:, at], sent.at[3],
               pass_recv.at[core, d] if d == h else end_recv, dev(to[d], groups[p])).start()

    mine = place(core, t, 0, block)
    for p in both:
        for d in (RIGHT, LEFT):
            i = d * 2 + p
            with jax.named_scope(f"near{d}{p}"):
                take(near_recv.at[i], 2 * T)
            yb[p, :, d * T : (d + 1) * T] = (
                ysum[p, :, d * T : (d + 1) * T] + near_in[i, 0].astype(F32) + near_in[i, 1].astype(F32)).astype(BF16)
            share(p, d, d)
        for d in (RIGHT, LEFT):
            share(p, d, 1 - d)
    y_ref[:, mine] = yb[core]
    remote(yb.at[1 - core], y_ref.at[:, mine], sent.at[3], end_recv, dev(t, other)).start()

    for p in both:
        for d in (RIGHT, LEFT):
            with jax.named_scope(f"pass{d}{p}"):
                take(pass_recv.at[p, d], T)
            at = place(p, (left, right)[d], d, T)
            remote(y_ref.at[:, at], y_ref.at[:, at], sent.at[4], end_recv, dev(to[d], g)).start()
    with jax.named_scope("end"):
        take(end_recv, 8 * T + block)
    with jax.named_scope("sends"):
        for i, width in enumerate((depth, 2 * half, 12 * T, 8 * T + block, 4 * T)):
            take(sent.at[i], width)


def solution(mesh):
    n = mesh.shape["tp"]

    def step(x, w_gate, w_up, w_down):
        rows, depth = x.shape
        hidden, out = w_down.shape
        steps, block = hidden // 2 // T, out // 2 // n
        hbm = pl.BlockSpec(memory_space=pl.ANY)
        return pl.pallas_call(
            functools.partial(kernel, n),
            out_shape=pltpu.VMEM((rows, out), BF16),
            in_specs=[hbm] * 4,
            out_specs=pl.BlockSpec(memory_space=pltpu.VMEM),
            scratch_shapes=[
                pltpu.VMEM((2, rows, depth), BF16),
                pltpu.VMEM((steps, depth, 2 * T), BF16),
                pltpu.VMEM((n, hidden, block), BF16),
                pltpu.VMEM((2, rows, 2 * T), F32),
                pltpu.VMEM((2, rows, hidden), BF16),
                pltpu.VMEM((2, rows, block), F32),
                pltpu.VMEM((2, rows, block), F32),
                pltpu.VMEM((2, 2, rows, T), F32),
                pltpu.VMEM((12, rows, T), BF16),
                pltpu.VMEM((4, rows, T), BF16),
                pltpu.VMEM((4, 2, rows, T), BF16),
                pltpu.VMEM((2, rows, block), BF16),
                pltpu.SemaphoreType.REGULAR,
            ],
            compiler_params=pltpu.CompilerParams(
                collective_id=0, has_side_effects=True, vmem_limit_bytes=56 * 1024 * 1024
            ),
        )(x, w_gate, w_up, w_down)

    return jax.shard_map(
        step,
        mesh=mesh,
        in_specs=(P("dp", None), P(None, "tp"), P(None, "tp"), P("tp", None)),
        out_specs=P("dp", None),
        check_vma=False,
    )
```

```python
import functools

import jax
import jax.numpy as jnp
from jax import lax
from jax.experimental import pallas as pl
from jax.experimental.pallas import tpu as pltpu
from jax.sharding import PartitionSpec as P

MESH = pl.DeviceIdType.MESH
BF16 = jnp.bfloat16
F32 = jnp.float32
T = 256
Q = 4
FAR, NEAR, CARRY = 0, 1, 2
RIGHT, LEFT = 0, 1


def kernel(n, *refs):
    DMA = pltpu.SemaphoreType.DMA
    steps = refs[1].shape[1] // 2 // T
    pl.run_scoped(
        functools.partial(body, n, *refs),
        DMA((Q,)), DMA((steps + 1,)), DMA((n,)), DMA((5,)),
        DMA, DMA((2, 2)), DMA((4,)), DMA((4,)), DMA((2, 2)), DMA,
    )


def body(
    n, x_hbm, wg_hbm, wu_hbm, wd_hbm, y_ref,
    xv, wgu, wd, gacc, hid, far_sum, ysum, carry, stage, far_in, near_in, yb,
    met, x_sem, w_sem, d_sem, sent, x_recv, h_recv, far_recv, near_recv, pass_recv, end_recv,
):
    t = lax.axis_index("tp")
    g = lax.axis_index("dp")
    core = lax.rem(g, 2)
    groups = (g - core, g - core + 1)
    other = g + 1 - 2 * core
    right, left = lax.rem(t + 1, n), lax.rem(t + n - 1, n)
    far = lax.rem(t + 2, n)
    rows, depth = x_hbm.shape
    half = wg_hbm.shape[1] // 2
    steps = half // T
    cols = wd_hbm.shape[1] // 2
    block = cols // n
    to = (right, left)

    def dev(tp, dp):
        return {"tp": tp, "dp": dp}

    def remote(src, dst, send, rcv, device):
        return pltpu.make_async_remote_copy(
            src_ref=src, dst_ref=dst, send_sem=send, recv_sem=rcv,
            device_id=device, device_id_type=MESH,
        )

    def start(copies):
        for copy in copies:
            copy.start(priority=1)

    def wait(copies, name):
        with jax.named_scope(name):
            for copy in copies:
                copy.wait()

    deep = [pl.ds(k * (depth // Q), depth // Q) for k in range(Q)]
    x_loads = [pltpu.make_async_copy(x_hbm.at[:, at], xv.at[core, :, at], x_sem.at[k]) for k, at in enumerate(deep)]
    for copy in x_loads:
        copy.start()
    upper, lower, full = pl.ds(0, depth // 2), pl.ds(depth // 2, depth // 2), pl.ds(0, depth)
    parts = [(j, at) for j in range(steps) for at in ((upper, lower) if j == 1 else (full,))]
    for i, (j, at) in enumerate(parts):
        start([pltpu.make_async_copy(
            w.at[at, pl.ds(pl.multiple_of(core * half + j * T, T), T)], wgu.at[j, at, pl.ds(q * T, T)], w_sem.at[i])
            for q, w in enumerate((wg_hbm, wu_hbm))])

    def load(i):
        j, at = parts[i]
        wait([pltpu.make_async_copy(wg_hbm.at[at, pl.ds(0, 2 * T)], wgu.at[j, at, :], w_sem.at[i])], f"w{i}")

    def take(sem, width):
        at = pl.ds(0, width)
        pltpu.make_async_copy(x_hbm.at[:, at], xv.at[0, :, at], sem).wait()

    d_loads = []
    for s, owner in enumerate((far, right, left, t)):
        at = pl.ds(pl.multiple_of(core * cols + owner * block, block), block)
        d_loads.append([
            pltpu.make_async_copy(
                wd_hbm.at[pl.ds(pl.multiple_of(c * half, half), half), at],
                wd.at[s, pl.ds(i * half, half), :], d_sem.at[s])
            for i, c in enumerate((core, 1 - core))])

    def load_down(s):
        wait([pltpu.make_async_copy(wd_hbm.at[:, pl.ds(0, block)], wd.at[s], d_sem.at[s])], f"d{s}")

    barrier = pltpu.get_barrier_semaphore()

    def signal(sem, device):
        pl.semaphore_signal(sem, inc=1, device_id=device, device_id_type=MESH)

    @pl.when(core == 0)
    def _():
        signal(barrier, dev(t, other))

    @pl.when(core == 1)
    def _():
        pl.semaphore_wait(barrier, 1)
        signal(met, dev(t, other))


    @pl.when(core == 0)
    def _():
        pl.semaphore_wait(met, 1)
        for a in to:
            signal(barrier, dev(a, g))

    for k, at in enumerate(deep):
        wait([x_loads[k]], "xl")
        remote(xv.at[core, :, at], xv.at[core, :, at], sent.at[0], x_recv, dev(t, other)).start()

    def dot(a, b):
        return jnp.dot(a, b, preferred_element_type=F32)

    def gate_up(j, p, at=slice(None)):
        return dot(xv[p, :, at], wgu[j, at, :])

    last = steps - 1

    def activate(j, p, a):
        hid[p, :, j * T : (j + 1) * T] = (jax.nn.gelu(a[:, :T]) * a[:, T:]).astype(BF16)

    def give(j, p):
        remote(
            hid.at[p, :, pl.ds(j * T, T)], hid.at[p, :, pl.ds(half + j * T, T)],
            sent.at[1], h_recv.at[p, int(j >= last - p)], dev(t, other)).start()

    both = (0, 1)
    load(0)
    gacc[0] = gate_up(0, core)
    load(1)
    gacc[1] = gate_up(1, core, slice(0, depth // 2))
    load(2)
    with jax.named_scope("x"):
        take(x_recv, depth)
    activate(0, core, gacc[0])
    activate(0, 1 - core, gate_up(0, 1 - core))
    activate(1, core, gacc[1] + gate_up(1, core, slice(depth // 2, depth)))
    activate(1, 1 - core, gate_up(1, 1 - core))
    for j in (0, 1):
        for p in both:
            give(j, p)
    for j in range(2, last - 1):
        load(j + 1)
        start(d_loads[j - 2])
        a = dot(xv[...].reshape(2 * rows, depth), wgu[j])
        for p in both:
            activate(j, p, a[p * rows : (p + 1) * rows])
        for p in both:
            give(j, p)

    @pl.when(core == 0)
    def _():
        pl.semaphore_wait(barrier, 2)
        signal(met, dev(t, other))

    load(last)
    for s in range(last - 3, n):
        start(d_loads[s])
    activate(last - 1, 0, gate_up(last - 1, 0))
    give(last - 1, 0)
    load(last + 1)
    activate(last, 0, gate_up(last, 0))
    give(last, 0)
    gacc[0] = gate_up(last - 1, 1, slice(0, depth // 2))

    @pl.when(core == 1)
    def _():
        pl.semaphore_wait(met, 1)

    def hop(kind, d, rs):
        dst, sem = {
            FAR: (far_in.at[d * 2 + rs], far_recv.at[d * 2 + rs]),
            CARRY: (near_in.at[d * 2 + rs, 0], near_recv.at[d * 2 + rs]),
            NEAR: (near_in.at[(1 - d) * 2 + rs, 1], near_recv.at[(1 - d) * 2 + rs]),
        }[kind]
        return remote(stage.at[(kind * 2 + d) * 2 + rs], dst, sent.at[2], sem, dev(to[d], g))

    def put(kind, d, rs, v):
        stage[(kind * 2 + d) * 2 + rs] = v.astype(BF16)

    def send(kind, d, rs):
        hop(kind, d, rs).start()


    def far_block(p):
        with jax.named_scope(f"h{p}"):
            take(h_recv.at[p, 0], (last - p) * T)
        most = 2 * half - (1 + p) * T
        far_sum[p] = dot(hid[p, :, :most], wd[0, :most, :])
        with jax.named_scope(f"hl{p}"):
            take(h_recv.at[p, 1], (1 + p) * T)
        v = far_sum[p] + dot(hid[p, :, most:], wd[0, most:, :])
        for d in (RIGHT, LEFT):
            put(FAR, d, p, v[:, d * T : (d + 1) * T])
        for d in (RIGHT, LEFT):
            send(FAR, d, p)

    def down(s, p, d):
        return dot(hid[p], wd[s, :, d * T : (d + 1) * T])

    load_down(0)
    far_block(0)
    load_down(1)
    load_down(2)
    activate(last - 1, 1, gacc[0] + gate_up(last - 1, 1, slice(depth // 2, depth)))
    activate(last, 1, gate_up(last, 1))
    for d in (RIGHT, LEFT):
        put(NEAR, d, 0, down(1 + d, 0, 1 - d))
    give(last - 1, 1)
    give(last, 1)
    for d in (RIGHT, LEFT):
        send(NEAR, d, 0)
    for d in (RIGHT, LEFT):
        carry[d, 0] = down(1 + d, 0, d)
    far_block(1)
    for d in (RIGHT, LEFT):
        carry[d, 1] = down(1 + d, 1, d)
        put(NEAR, d, 1, down(1 + d, 1, 1 - d))
    for p in both:
        for d in (RIGHT, LEFT):
            with jax.named_scope(f"far{d}{p}"):
                take(far_recv.at[d * 2 + p], T)
            put(CARRY, d, p, carry[d, p] + far_in[d * 2 + p].astype(F32))
            send(CARRY, d, p)
        if p == 0:
            for d in (RIGHT, LEFT):
                send(NEAR, d, 1)
            load_down(3)
            v = dot(hid[...].reshape(2 * rows, 2 * half), wd[3])
            for r in both:
                ysum[r] = v[r * rows : (r + 1) * rows]

    def place(k, owner, h, width):
        return pl.ds(pl.multiple_of(k * cols + owner * block + h * T, T), width)

    def share(p, d, h):
        at = place(core, t, h, T)
        remote(yb.at[p, :, pl.ds(h * T, T)], y_ref.at[:, at], sent.at[3],
               pass_recv.at[core, d] if d == h else end_recv, dev(to[d], groups[p])).start()

    mine = place(core, t, 0, block)
    for p in both:
        for d in (RIGHT, LEFT):
            i = d * 2 + p
            with jax.named_scope(f"near{d}{p}"):
                take(near_recv.at[i], 2 * T)
            yb[p, :, d * T : (d + 1) * T] = (
                ysum[p, :, d * T : (d + 1) * T] + near_in[i, 0].astype(F32) + near_in[i, 1].astype(F32)).astype(BF16)
            share(p, d, d)
        for d in (RIGHT, LEFT):
            share(p, d, 1 - d)
    y_ref[:, mine] = yb[core]
    remote(yb.at[1 - core], y_ref.at[:, mine], sent.at[3], end_recv, dev(t, other)).start()

    for p in both:
        for d in (RIGHT, LEFT):
            with jax.named_scope(f"pass{d}{p}"):
                take(pass_recv.at[p, d], T)
            at = place(p, (left, right)[d], d, T)
            remote(y_ref.at[:, at], y_ref.at[:, at], sent.at[4], end_recv, dev(to[d], g)).start()
    with jax.named_scope("end"):
        take(end_recv, 8 * T + block)
    with jax.named_scope("sends"):
        for i, width in enumerate((depth, 2 * half, 12 * T, 8 * T + block, 4 * T)):
            take(sent.at[i], width)


def solution(mesh):
    n = mesh.shape["tp"]

    def step(x, w_gate, w_up, w_down):
        rows, depth = x.shape
        hidden, out = w_down.shape
        steps, block = hidden // 2 // T, out // 2 // n
        hbm = pl.BlockSpec(memory_space=pl.ANY)
        return pl.pallas_call(
            functools.partial(kernel, n),
            out_shape=pltpu.VMEM((rows, out), BF16),
            in_specs=[hbm] * 4,
            out_specs=pl.BlockSpec(memory_space=pltpu.VMEM),
            scratch_shapes=[
                pltpu.VMEM((2, rows, depth), BF16),
                pltpu.VMEM((steps, depth, 2 * T), BF16),
                pltpu.VMEM((n, hidden, block), BF16),
                pltpu.VMEM((2, rows, 2 * T), F32),
                pltpu.VMEM((2, rows, hidden), BF16),
                pltpu.VMEM((2, rows, block), F32),
                pltpu.VMEM((2, rows, block), F32),
                pltpu.VMEM((2, 2, rows, T), F32),
                pltpu.VMEM((12, rows, T), BF16),
                pltpu.VMEM((4, rows, T), BF16),
                pltpu.VMEM((4, 2, rows, T), BF16),
                pltpu.VMEM((2, rows, block), BF16),
                pltpu.SemaphoreType.REGULAR,
            ],
            compiler_params=pltpu.CompilerParams(
                collective_id=0, has_side_effects=True, vmem_limit_bytes=56 * 1024 * 1024
            ),
        )(x, w_gate, w_up, w_down)

    return jax.shard_map(
        step,
        mesh=mesh,
        in_specs=(P("dp", None), P(None, "tp"), P(None, "tp"), P("tp", None)),
        out_specs=P("dp", None),
        check_vma=False,
    )
```
